32 devices in a mesh: node: 16 (over z, y, core), blk: 2 (over x).
Axes of the slice: x: 2, y: 2, z: 4, core: 2. Of those that a mesh axis runs over, the one named last changes fastest.
Arguments:
- params: bfloat16 [16, 128, 14336], P('node', 'blk'), may hold values from -40 to 40
- weights: int32 [16], P('node'), may hold values from 1 to 8
Outputs:
- debiased: float32 [16, 128, 14336], P('node', 'blk')
- average: float32 [128, 14336], P('blk', 'node')
- spread: float32 [16], P('node')
The draws below stay inside these ranges and needn't reach their ends.
All inputs are finite; a program needn't handle non-finite values.
Results may differ from the reference program's by a relative error of at most 0.0003.
Values may be sent and summed in bfloat16 or wider, within the bound.
A program may use at most 64 MiB of HBM per device.

```python
import jax
import jax.numpy as jnp

FF = 14336
ROUNDS = 3
ROWS = 128
NODES = 16


def draw_params(key, part):
    keys = jax.random.split(jax.random.fold_in(key, 11), 3)
    index = jnp.arange(NODES, dtype=jnp.float32)
    node_scale = (1.0 + 2.0 * index / max(NODES - 1, 1)) * jax.random.uniform(keys[1], (NODES,), minval=0.8, maxval=1.2)
    base = jax.random.normal(keys[0], (NODES, ROWS, FF))
    row_scale = jnp.exp(jax.random.uniform(keys[2], (ROWS,), minval=0.0, maxval=jnp.log(3.0)))
    values = base * node_scale[:, None, None] * row_scale[None, :, None]
    return jnp.clip(values, -40.0, 40.0).astype(jnp.bfloat16)


def touch_ends(entries, key, least, largest):
    extent = entries.shape
    spot = [jax.random.randint(jax.random.fold_in(key, axis), (), 0, extent[axis]) for axis in range(len(extent))]
    entries = entries.at[tuple(spot)].set(least)
    longest = extent.index(max(extent))
    spot[longest] = (spot[longest] + 1) % extent[longest]
    return entries.at[tuple(spot)].set(largest)


def setup_inputs(seed: int = 0) -> dict:
    streams_of = jax.random.split(jax.random.key(seed), 3)
    return {
        "params": draw_params(jax.random.fold_in(streams_of[2], 71), 0),
        "weights": touch_ends(jax.random.randint(streams_of[1], (NODES,), 1, 9), jax.random.fold_in(streams_of[1], 1), 1, 8).astype(jnp.int32),
    }


def reference(params, weights):
    scale0 = weights.astype(jnp.float32)
    value = scale0[:, None, None] * params.astype(jnp.float32)
    scale = scale0
    levels = NODES.bit_length() - 1
    for step in range(ROUNDS):
        hop = 1 << (step % levels)
        value = 0.5 * value + 0.5 * jnp.roll(value, hop, 0)
        scale = 0.5 * scale + 0.5 * jnp.roll(scale, hop, 0)
    debiased = value / scale[:, None, None]
    numer = jnp.sum(scale0[:, None, None] * params.astype(jnp.float32), axis=0)
    average = numer / jnp.sum(scale0)
    spread = jnp.sum((debiased - average[None]) ** 2, axis=(1, 2)) / (ROWS * FF)
    return debiased, average, spread
```

```python
import functools

import jax
import jax.numpy as jnp
from jax import lax
from jax.experimental import pallas as pl
from jax.experimental.pallas import tpu as pltpu
from jax.sharding import PartitionSpec as P

ROUNDS = 3
GROUP = 4
LEVELS = 4
SPLIT = 2
LANES = 128


def kernel(p_ref, w_ref, out_ref, avg_ref, spread_ref,
           raw_own, raw_a, raw_b, raw_c, q_a, q_b, q_send, dbuf, avgbuf,
           wts, acc, spread_in, spread_part, spread_x,
           near_send, near_recv, own_sem, far_send, far_recv, back_send, back_recv,
           back_own, w_send, w_recv, s_send, s_recv, avg_sem):
    node = lax.axis_index("node")
    side = lax.axis_index("blk")
    z = node // GROUP
    r = node % GROUP
    half, core = r // 2, r % 2
    rows, width = raw_own.shape[2], raw_own.shape[3]
    chunks = raw_own.shape[0]
    hidden = p_ref.shape[2]
    row_total = p_ref.shape[1] * lax.axis_size("blk")

    def peer(o):
        y = 1 - half if o & 2 else half
        c = 1 - core if o & 1 else core
        return y * 2 + c

    def dev(zz, rr):
        return {"node": zz * GROUP + rr}

    inner = jnp.logical_and(z >= 1, z <= 2)
    outer = jnp.logical_not(inner)
    mate = 3 - z
    nb = (z // 2) * 2 + 1 - z % 2
    inner_count = (1 - z // 3) * ((z + 2) // 3)
    opposite = (z + 2) % LEVELS
    behind = (z + 3) % LEVELS

    def remote(src, dst, ssem, rsem, device):
        return pltpu.make_async_remote_copy(
            src_ref=src, dst_ref=dst, send_sem=ssem, recv_sem=rsem,
            device_id=device, device_id_type=pl.DeviceIdType.MESH)

    wts[z, r] = jnp.full((8, LANES), w_ref[0].astype(jnp.float32))
    acc[...] = jnp.zeros_like(acc)

    def own_slice(k):
        return pl.ds((k % SPLIT) * rows, rows)

    def block(k, rr):
        return pl.ds(pl.multiple_of(((k // SPLIT) * GROUP + rr) * width, LANES), width)

    locals_in = []
    for k in range(chunks):
        locals_in.append(pltpu.make_async_copy(
            p_ref.at[0, own_slice(k), block(k, r)], raw_own.at[k, r], own_sem.at[k]))
        locals_in[-1].start()

    barrier = pltpu.get_barrier_semaphore()

    def greet(device):
        pl.semaphore_signal(barrier, inc=1, device_id=device,
                            device_id_type=pl.DeviceIdType.MESH)

    for o in (1, 2, 3):
        greet(dev(z, peer(o)))
    greet({"blk": 1 - side})
    greet(dev(nb, r))

    @pl.when(inner)
    def _():
        greet(dev(mate, r))

    pl.semaphore_wait(barrier, 5 + inner_count)

    def w_near(o):
        return remote(wts.at[z, r], wts.at[z, r], w_send.at[o - 1], w_recv.at[o - 1],
                      dev(z, peer(o)))

    def near(k, o):
        return remote(p_ref.at[0, own_slice(k), block(k, peer(o))], raw_own.at[k, r],
                      near_send.at[k, o - 1], near_recv.at[k, o - 1], dev(z, peer(o)))

    for o in (1, 2, 3):
        w_near(o).start()
    for k in range(chunks):
        for o in (2, 3, 1):
            near(k, o).start()

    arrived = set()

    def wait_own(k):
        if k in arrived:
            return
        arrived.add(k)
        locals_in[k].wait()
        for o in (1, 2, 3):
            near(k, o).wait_recv()

    def row(zz, i):
        return wts[zz, i, 0:1, :]

    def f32(ref, k, i, cols):
        return ref[k, i, :, cols].astype(jnp.float32)

    def group_sum(ref, k, zz, cols):
        total = f32(ref, k, 0, cols) * row(zz, 0)
        for i in range(1, GROUP):
            total = total + f32(ref, k, i, cols) * row(zz, i)
        return total

    def columns(j):
        return pl.ds(pl.multiple_of(j * LANES, LANES), LANES)

    def back(k, o):
        return remote(dbuf.at[k, peer(o)], out_ref.at[0, own_slice(k), block(k, r)],
                      back_send.at[k, o - 1], back_recv.at[k, o - 1], dev(z, peer(o)))

    def back_local(k):
        return pltpu.make_async_copy(
            dbuf.at[k, r], out_ref.at[0, own_slice(k), block(k, r)], back_own.at[k])

    def group_weight(zz):
        return row(zz, 0) + row(zz, 1) + row(zz, 2) + row(zz, 3)

    def finish(k, is_inner):
        far = raw_c if is_inner else raw_a
        at_one = (z == 1)
        at_zero = (z == 0)
        s0, s1 = row(z, 0), row(z, 0) + row(z, 1)
        s2 = s1 + row(z, 2)
        s3 = s2 + row(z, 3)
        t3 = row(opposite, 3)
        t2 = t3 + row(opposite, 2)
        t1 = t2 + row(opposite, 1)
        sb = group_weight(behind)
        scales = (1.0 / (s0 + sb + t1), 1.0 / (s1 + sb + t2), 1.0 / (s2 + sb + t3),
                  1.0 / (s3 + sb))
        whole = 1.0 / (group_weight(0) + group_weight(1) + group_weight(2) + group_weight(3))

        def step(j, sums):
            cols = columns(j)
            v0 = f32(raw_own, k, 0, cols) * row(z, 0)
            v1 = v0 + f32(raw_own, k, 1, cols) * row(z, 1)
            v2 = v1 + f32(raw_own, k, 2, cols) * row(z, 2)
            v3 = v2 + f32(raw_own, k, 3, cols) * row(z, 3)
            u3 = f32(far, k, 3, cols) * row(opposite, 3)
            u2 = u3 + f32(far, k, 2, cols) * row(opposite, 2)
            u1 = u2 + f32(far, k, 1, cols) * row(opposite, 1)
            u0 = u1 + f32(far, k, 0, cols) * row(opposite, 0)
            if is_inner:
                q_send[k, 1, :, cols] = u0
                qo = group_sum(raw_a, k, nb, cols)
                qj = group_sum(raw_b, k, mate, cols)
                prior = jnp.where(at_one, qo, qj)
                total = v3 + u0 + qo + qj
            else:
                qi = q_a[k, :, cols]
                qx = q_b[k, :, cols]
                prior = jnp.where(at_zero, qx, qi)
                total = v3 + u0 + qi + qx
            mean = total * whole
            avgbuf[k // SPLIT, own_slice(k), cols] = mean
            fresh = []
            for i, value in enumerate((v0 + u1, v1 + u2, v2 + u3, v3)):
                d = (value + prior) * scales[i]
                dbuf[k, i, :, cols] = d
                gap = d - mean
                gap = gap * gap
                part = gap[0:8]
                for e in range(8, rows, 8):
                    part = part + gap[e:e + 8]
                fresh.append(sums[i] + part)
            return tuple(fresh)

        zero = jnp.zeros((8, LANES), jnp.float32)
        sums = lax.fori_loop(0, width // LANES, step, (zero,) * GROUP)
        for i in range(GROUP):
            acc[i] += sums[i]

    def send_back(k):
        for o in (2, 3, 1):
            back(k, o).start()
        back_local(k).start()

    def to_inner(k):
        return remote(raw_own.at[k], raw_a.at[k], far_send.at[k, 0], far_recv.at[k, 0],
                      dev(nb, r))

    def across(k):
        return remote(raw_own.at[k], raw_b.at[k], far_send.at[k, 0], far_recv.at[k, 1],
                      dev(mate, r))

    def across_relay(k):
        return remote(raw_a.at[k], raw_c.at[k], far_send.at[k, 1], far_recv.at[k, 2],
                      dev(mate, r))

    def outward_relay(k):
        return remote(raw_b.at[k], raw_a.at[k], far_send.at[k, 2], far_recv.at[k, 0],
                      dev(nb, r))

    def outward_q(k, which):
        dst = q_b if which else q_a
        return remote(q_send.at[k, which], dst.at[k], far_send.at[k, 3 + which],
                      far_recv.at[k, 3 + which], dev(nb, r))

    def w_copy(level, slot, target):
        return remote(wts.at[level], wts.at[level], w_send.at[slot], w_recv.at[slot],
                      dev(target, r))

    def wait_weights():
        for o in (1, 2, 3):
            w_near(o).wait_recv()

    @pl.when(inner)
    def _():
        arrived.clear()

        def group_out(k):
            wait_own(k)

            def step(j, carry):
                cols = columns(j)
                q_send[k, 0, :, cols] = group_sum(raw_own, k, z, cols)
                return carry

            lax.fori_loop(0, width // LANES, step, 0)
            outward_q(k, 0).start()

        wait_weights()
        w_copy(z, 3, nb).start()
        w_copy(z, 4, mate).start()
        for t in range(chunks + 2):
            if t < chunks:
                wait_own(t)
                across(t).start()
            for k in ((0,) if t == 0 else (2 * t - 1, 2 * t)):
                if k < chunks:
                    group_out(k)
            if t == 1:
                w_copy(nb, 3, nb).wait_recv()
                w_copy(nb, 5, mate).start()
                w_copy(z, 4, mate).wait_recv()
                w_copy(mate, 6, nb).start()
            k = t - 1
            if 0 <= k < chunks:
                across_in = to_inner(k)
                across_in.wait_recv()
                across_relay(k).start()
                across(k).wait_recv()
                outward_relay(k).start()
            if t == 2:
                w_copy(nb, 5, mate).wait_recv()
                w_copy(opposite, 7, nb).start()
            k = t - 2
            if 0 <= k < chunks:
                across_relay(k).wait_recv()
                finish(k, True)
                send_back(k)
                outward_q(k, 1).start()
        for k in range(chunks):
            across(k).wait_send()
            across_relay(k).wait_send()
            outward_relay(k).wait_send()
            outward_q(k, 0).wait_send()
            outward_q(k, 1).wait_send()
        w_copy(z, 3, nb).wait_send()
        w_copy(z, 4, mate).wait_send()
        w_copy(nb, 5, mate).wait_send()
        w_copy(mate, 6, nb).wait_send()
        w_copy(opposite, 7, nb).wait_send()

    @pl.when(outer)
    def _():
        arrived.clear()
        wait_weights()
        w_copy(z, 3, nb).start()
        for k in range(chunks):
            wait_own(k)
            to_inner(k).start()
        w_copy(nb, 3, nb).wait_recv()
        w_copy(opposite, 6, nb).wait_recv()
        w_copy(mate, 7, nb).wait_recv()
        for k in range(chunks):
            outward_q(k, 0).wait_recv()
            outward_relay(k).wait_recv()
            outward_q(k, 1).wait_recv()
            finish(k, False)
            send_back(k)
        for k in range(chunks):
            to_inner(k).wait_send()
        w_copy(z, 3, nb).wait_send()

    average = pltpu.make_async_copy(avgbuf.at[z], avg_ref, avg_sem)
    average.start()

    def share(o):
        return remote(acc.at[peer(o)], spread_in.at[o - 1], s_send.at[o - 1],
                      s_recv.at[o - 1], dev(z, peer(o)))

    for o in (1, 2, 3):
        share(o).start()
    for o in (1, 2, 3):
        share(o).wait_recv()
    spread_part[...] = acc[r] + spread_in[0] + spread_in[1] + spread_in[2]
    swap = remote(spread_part, spread_x, s_send.at[3], s_recv.at[3], {"blk": 1 - side})
    swap.start()
    for k in range(chunks):
        for o in (1, 2, 3):
            near(k, o).wait_send()
            back(k, o).wait()
        back_local(k).wait()
    for o in (1, 2, 3):
        w_near(o).wait_send()
        share(o).wait_send()
    average.wait()
    swap.wait()
    spread_ref[0] = jnp.sum(spread_part[...] + spread_x[...]) / (row_total * hidden)


def fused(params, weights):
    _, rows, hidden = params.shape
    node_count = lax.axis_size("node")
    width = hidden // node_count
    piece = rows // SPLIT
    chunks = LEVELS * SPLIT
    raw = pltpu.VMEM((chunks, GROUP, piece, width), params.dtype)
    q = pltpu.VMEM((chunks, piece, width), jnp.float32)
    tile = pltpu.VMEM((8, LANES), jnp.float32)
    dma = pltpu.SemaphoreType.DMA
    debiased, average, spread = pl.pallas_call(
        kernel,
        out_shape=(
            jax.ShapeDtypeStruct((1, rows, hidden), jnp.float32),
            jax.ShapeDtypeStruct((rows, width), jnp.float32),
            jax.ShapeDtypeStruct((1,), jnp.float32),
        ),
        in_specs=[pl.BlockSpec(memory_space=pl.ANY), pl.BlockSpec(memory_space=pltpu.SMEM)],
        out_specs=(pl.BlockSpec(memory_space=pl.ANY), pl.BlockSpec(memory_space=pl.ANY),
                   pl.BlockSpec(memory_space=pltpu.SMEM)),
        scratch_shapes=[
            raw, raw, raw, raw, q, q,
            pltpu.VMEM((chunks, 2, piece, width), jnp.float32),
            pltpu.VMEM((chunks, GROUP, piece, width), jnp.float32),
            pltpu.VMEM((LEVELS, rows, width), jnp.float32),
            pltpu.VMEM((LEVELS, GROUP, 8, LANES), jnp.float32),
            pltpu.VMEM((GROUP, 8, LANES), jnp.float32),
            pltpu.VMEM((3, 8, LANES), jnp.float32),
            tile, tile,
            dma((chunks, 3)), dma((chunks, 3)), dma((chunks,)),
            dma((chunks, 5)), dma((chunks, 5)),
            dma((chunks, 3)), dma((chunks, 3)), dma((chunks,)),
            dma((8,)), dma((8,)), dma((4,)), dma((4,)), dma,
        ],
        compiler_params=pltpu.CompilerParams(
            collective_id=0, has_side_effects=True, vmem_limit_bytes=56 << 20),
    )(params, weights)
    return debiased, average, spread


def from_behind(value, axis, steps):
    count = lax.axis_size(axis)
    pairs = [(source, (source + steps) % count) for source in range(count)]
    return lax.ppermute(value, axis, pairs)


def push_round(value, scale, hop):
    received = from_behind((value, scale), "node", hop)
    return (received[0], received[1])


def shards(params, weights):
    node_count = lax.axis_size("node")
    levels = node_count.bit_length() - 1
    scale0 = weights.astype(jnp.float32)
    weighted = scale0[:, None, None] * params.astype(jnp.float32)
    value = weighted
    scale = scale0
    for step in range(ROUNDS):
        hop = 1 << step % levels
        if step == 0:
            raw = from_behind((params, weights.astype(jnp.bfloat16)), "node", hop)
            other_scale = raw[1].astype(jnp.float32)
            other_value = other_scale[:, None, None] * raw[0].astype(jnp.float32)
        else:
            other_value, other_scale = push_round(value, scale, hop)
        value = 0.5 * value + 0.5 * other_value
        scale = 0.5 * scale + 0.5 * other_scale
    debiased = value / scale[:, None, None]
    hidden_units = params.shape[2]
    width = hidden_units // node_count
    local = debiased[0]
    numer, total = lax.psum((weighted[0], jnp.sum(scale0)), "node")
    whole = numer / total
    partial_value = jnp.sum((local - whole) ** 2)[None]
    average = lax.dynamic_slice_in_dim(whole, lax.axis_index("node") * width, width, 1)
    row_count = params.shape[1] * lax.axis_size("blk")
    spread = lax.psum(partial_value, "blk") / (row_count * hidden_units)
    return (debiased, average, spread)


def solution(mesh):
    line = mesh.shape["node"] == GROUP * LEVELS and mesh.shape["blk"] == 2
    return jax.shard_map(
        fused if line else shards,
        mesh=mesh,
        in_specs=(P("node", "blk", None), P("node")),
        out_specs=(P("node", "blk", None), P("blk", "node"), P("node")),
        check_vma=False,
    )
```

```python
import functools

import jax
import jax.numpy as jnp
from jax import lax
from jax.experimental import pallas as pl
from jax.experimental.pallas import tpu as pltpu
from jax.sharding import PartitionSpec as P

ROUNDS = 3
GROUP = 4
LEVELS = 4
SPLIT = 4
LANES = 128


def kernel(p_ref, w_ref, out_ref, avg_ref, spread_ref,
           raw_own, raw_a, raw_b, raw_c, q_a, q_b, q_send, dbuf, avgbuf,
           wts, acc, spread_in, spread_part, spread_x,
           near_send, near_recv, own_sem, far_send, far_recv, back_send, back_recv,
           back_own, w_send, w_recv, s_send, s_recv, avg_sem):
    node = lax.axis_index("node")
    side = lax.axis_index("blk")
    z = node // GROUP
    r = node % GROUP
    half, core = r // 2, r % 2
    rows, width = raw_own.shape[2], raw_own.shape[3]
    chunks = raw_own.shape[0]
    hidden = p_ref.shape[2]
    row_total = p_ref.shape[1] * lax.axis_size("blk")

    def peer(o):
        y = 1 - half if o & 2 else half
        c = 1 - core if o & 1 else core
        return y * 2 + c

    def dev(zz, rr):
        return {"node": zz * GROUP + rr}

    inner = jnp.logical_and(z >= 1, z <= 2)
    outer = jnp.logical_not(inner)
    mate = 3 - z
    nb = (z // 2) * 2 + 1 - z % 2
    inner_count = (1 - z // 3) * ((z + 2) // 3)
    opposite = (z + 2) % LEVELS
    behind = (z + 3) % LEVELS

    def remote(src, dst, ssem, rsem, device):
        return pltpu.make_async_remote_copy(
            src_ref=src, dst_ref=dst, send_sem=ssem, recv_sem=rsem,
            device_id=device, device_id_type=pl.DeviceIdType.MESH)

    wts[z, r] = jnp.full((8, LANES), w_ref[0].astype(jnp.float32))
    acc[...] = jnp.zeros_like(acc)

    def own_slice(k):
        return pl.ds((k % SPLIT) * rows, rows)

    def block(k, rr):
        return pl.ds(pl.multiple_of(((k // SPLIT) * GROUP + rr) * width, LANES), width)

    locals_in = []
    for k in range(chunks):
        locals_in.append(pltpu.make_async_copy(
            p_ref.at[0, own_slice(k), block(k, r)], raw_own.at[k, r], own_sem.at[k]))
        locals_in[-1].start()

    barrier = pltpu.get_barrier_semaphore()

    def greet(device):
        pl.semaphore_signal(barrier, inc=1, device_id=device,
                            device_id_type=pl.DeviceIdType.MESH)

    for o in (1, 2, 3):
        greet(dev(z, peer(o)))
    greet({"blk": 1 - side})
    greet(dev(nb, r))

    @pl.when(inner)
    def _():
        greet(dev(mate, r))

    pl.semaphore_wait(barrier, 5 + inner_count)

    def w_near(o):
        return remote(wts.at[z, r], wts.at[z, r], w_send.at[o - 1], w_recv.at[o - 1],
                      dev(z, peer(o)))

    def near(k, o):
        return remote(p_ref.at[0, own_slice(k), block(k, peer(o))], raw_own.at[k, r],
                      near_send.at[k, o - 1], near_recv.at[k, o - 1], dev(z, peer(o)))

    for o in (1, 2, 3):
        w_near(o).start()
    for k in range(chunks):
        for o in (2, 3, 1):
            near(k, o).start()

    arrived = set()

    def wait_own(k):
        if k in arrived:
            return
        arrived.add(k)
        locals_in[k].wait()
        for o in (1, 2, 3):
            near(k, o).wait_recv()

    def row(zz, i):
        return wts[zz, i, 0:1, :]

    def f32(ref, k, i, cols):
        return ref[k, i, :, cols].astype(jnp.float32)

    def group_sum(ref, k, zz, cols):
        total = f32(ref, k, 0, cols) * row(zz, 0)
        for i in range(1, GROUP):
            total = total + f32(ref, k, i, cols) * row(zz, i)
        return total

    def columns(j):
        return pl.ds(pl.multiple_of(j * LANES, LANES), LANES)

    def back(k, o):
        return remote(dbuf.at[k, peer(o)], out_ref.at[0, own_slice(k), block(k, r)],
                      back_send.at[k, o - 1], back_recv.at[k, o - 1], dev(z, peer(o)))

    def back_local(k):
        return pltpu.make_async_copy(
            dbuf.at[k, r], out_ref.at[0, own_slice(k), block(k, r)], back_own.at[k])

    def group_weight(zz):
        return row(zz, 0) + row(zz, 1) + row(zz, 2) + row(zz, 3)

    def finish(k, is_inner):
        far = raw_c if is_inner else raw_a
        at_one = (z == 1)
        at_zero = (z == 0)
        s0, s1 = row(z, 0), row(z, 0) + row(z, 1)
        s2 = s1 + row(z, 2)
        s3 = s2 + row(z, 3)
        t3 = row(opposite, 3)
        t2 = t3 + row(opposite, 2)
        t1 = t2 + row(opposite, 1)
        sb = group_weight(behind)
        scales = (1.0 / (s0 + sb + t1), 1.0 / (s1 + sb + t2), 1.0 / (s2 + sb + t3),
                  1.0 / (s3 + sb))
        whole = 1.0 / (group_weight(0) + group_weight(1) + group_weight(2) + group_weight(3))

        def step(j, sums):
            cols = columns(j)
            v0 = f32(raw_own, k, 0, cols) * row(z, 0)
            v1 = v0 + f32(raw_own, k, 1, cols) * row(z, 1)
            v2 = v1 + f32(raw_own, k, 2, cols) * row(z, 2)
            v3 = v2 + f32(raw_own, k, 3, cols) * row(z, 3)
            u3 = f32(far, k, 3, cols) * row(opposite, 3)
            u2 = u3 + f32(far, k, 2, cols) * row(opposite, 2)
            u1 = u2 + f32(far, k, 1, cols) * row(opposite, 1)
            u0 = u1 + f32(far, k, 0, cols) * row(opposite, 0)
            if is_inner:
                q_send[k, 1, :, cols] = u0
                qo = group_sum(raw_a, k, nb, cols)
                qj = group_sum(raw_b, k, mate, cols)
                prior = jnp.where(at_one, qo, qj)
                total = v3 + u0 + qo + qj
            else:
                qi = q_a[k, :, cols]
                qx = q_b[k, :, cols]
                prior = jnp.where(at_zero, qx, qi)
                total = v3 + u0 + qi + qx
            mean = total * whole
            avgbuf[k // SPLIT, own_slice(k), cols] = mean
            fresh = []
            for i, value in enumerate((v0 + u1, v1 + u2, v2 + u3, v3)):
                d = (value + prior) * scales[i]
                dbuf[k, i, :, cols] = d
                gap = d - mean
                gap = gap * gap
                part = gap[0:8]
                for e in range(8, rows, 8):
                    part = part + gap[e:e + 8]
                fresh.append(sums[i] + part)
            return tuple(fresh)

        zero = jnp.zeros((8, LANES), jnp.float32)
        sums = lax.fori_loop(0, width // LANES, step, (zero,) * GROUP)
        for i in range(GROUP):
            acc[i] += sums[i]

    def share(o):
        return remote(acc.at[peer(o)], spread_in.at[o - 1], s_send.at[o - 1],
                      s_recv.at[o - 1], dev(z, peer(o)))

    def send_back(k):
        if k == chunks - 1:
            for o in (2, 3, 1):
                share(o).start()
        for o in (2, 3, 1):
            back(k, o).start()
        back_local(k).start()

    def to_inner(k):
        return remote(raw_own.at[k], raw_a.at[k], far_send.at[k, 0], far_recv.at[k, 0],
                      dev(nb, r))

    def across(k):
        return remote(raw_own.at[k], raw_b.at[k], far_send.at[k, 0], far_recv.at[k, 1],
                      dev(mate, r))

    def across_relay(k):
        return remote(raw_a.at[k], raw_c.at[k], far_send.at[k, 1], far_recv.at[k, 2],
                      dev(mate, r))

    def outward_relay(k):
        return remote(raw_b.at[k], raw_a.at[k], far_send.at[k, 2], far_recv.at[k, 0],
                      dev(nb, r))

    def outward_q(k, which):
        dst = q_b if which else q_a
        return remote(q_send.at[k, which], dst.at[k], far_send.at[k, 3 + which],
                      far_recv.at[k, 3 + which], dev(nb, r))

    def w_copy(level, slot, target):
        return remote(wts.at[level], wts.at[level], w_send.at[slot], w_recv.at[slot],
                      dev(target, r))

    def wait_weights():
        for o in (1, 2, 3):
            w_near(o).wait_recv()

    @pl.when(inner)
    def _():
        arrived.clear()

        def group_out(k):
            wait_own(k)

            def step(j, carry):
                cols = columns(j)
                q_send[k, 0, :, cols] = group_sum(raw_own, k, z, cols)
                return carry

            lax.fori_loop(0, width // LANES, step, 0)
            outward_q(k, 0).start()

        wait_weights()
        w_copy(z, 3, nb).start()
        w_copy(z, 4, mate).start()
        for t in range(chunks + 2):
            if t < chunks:
                wait_own(t)
                across(t).start()
            for k in ((0,) if t == 0 else (2 * t - 1, 2 * t)):
                if k < chunks:
                    group_out(k)
            if t == 1:
                w_copy(nb, 3, nb).wait_recv()
                w_copy(nb, 5, mate).start()
                w_copy(z, 4, mate).wait_recv()
                w_copy(mate, 6, nb).start()
            k = t - 1
            if 0 <= k < chunks:
                across_in = to_inner(k)
                across_in.wait_recv()
                across_relay(k).start()
                across(k).wait_recv()
                outward_relay(k).start()
            if t == 2:
                w_copy(nb, 5, mate).wait_recv()
                w_copy(opposite, 7, nb).start()
            k = t - 2
            if 0 <= k < chunks:
                across_relay(k).wait_recv()
                finish(k, True)
                outward_q(k, 1).start()
                send_back(k)
        for k in range(chunks):
            across(k).wait_send()
            across_relay(k).wait_send()
            outward_relay(k).wait_send()
            outward_q(k, 0).wait_send()
            outward_q(k, 1).wait_send()
        w_copy(z, 3, nb).wait_send()
        w_copy(z, 4, mate).wait_send()
        w_copy(nb, 5, mate).wait_send()
        w_copy(mate, 6, nb).wait_send()
        w_copy(opposite, 7, nb).wait_send()

    @pl.when(outer)
    def _():
        arrived.clear()
        wait_weights()
        w_copy(z, 3, nb).start()
        for k in range(chunks):
            wait_own(k)
            to_inner(k).start()
        w_copy(nb, 3, nb).wait_recv()
        w_copy(opposite, 6, nb).wait_recv()
        w_copy(mate, 7, nb).wait_recv()
        for k in range(chunks):
            outward_q(k, 0).wait_recv()
            outward_relay(k).wait_recv()
            outward_q(k, 1).wait_recv()
            finish(k, False)
            send_back(k)
        for k in range(chunks):
            to_inner(k).wait_send()
        w_copy(z, 3, nb).wait_send()

    average = pltpu.make_async_copy(avgbuf.at[z], avg_ref, avg_sem)
    average.start()

    for o in (1, 2, 3):
        share(o).wait_recv()
    spread_part[...] = acc[r] + spread_in[0] + spread_in[1] + spread_in[2]
    swap = remote(spread_part, spread_x, s_send.at[3], s_recv.at[3], {"blk": 1 - side})
    swap.start()
    for k in range(chunks):
        for o in (1, 2, 3):
            near(k, o).wait_send()
            back(k, o).wait()
        back_local(k).wait()
    for o in (1, 2, 3):
        w_near(o).wait_send()
        share(o).wait_send()
    average.wait()
    swap.wait()
    spread_ref[0] = jnp.sum(spread_part[...] + spread_x[...]) / (row_total * hidden)


def fused(params, weights):
    _, rows, hidden = params.shape
    node_count = lax.axis_size("node")
    width = hidden // node_count
    piece = rows // SPLIT
    chunks = LEVELS * SPLIT
    raw = pltpu.VMEM((chunks, GROUP, piece, width), params.dtype)
    q = pltpu.VMEM((chunks, piece, width), jnp.float32)
    tile = pltpu.VMEM((8, LANES), jnp.float32)
    dma = pltpu.SemaphoreType.DMA
    debiased, average, spread = pl.pallas_call(
        kernel,
        out_shape=(
            jax.ShapeDtypeStruct((1, rows, hidden), jnp.float32),
            jax.ShapeDtypeStruct((rows, width), jnp.float32),
            jax.ShapeDtypeStruct((1,), jnp.float32),
        ),
        in_specs=[pl.BlockSpec(memory_space=pltpu.HBM), pl.BlockSpec(memory_space=pltpu.SMEM)],
        out_specs=(pl.BlockSpec(memory_space=pl.ANY), pl.BlockSpec(memory_space=pl.ANY),
                   pl.BlockSpec(memory_space=pltpu.SMEM)),
        scratch_shapes=[
            raw, raw, raw, raw, q, q,
            pltpu.VMEM((chunks, 2, piece, width), jnp.float32),
            pltpu.VMEM((chunks, GROUP, piece, width), jnp.float32),
            pltpu.VMEM((LEVELS, rows, width), jnp.float32),
            pltpu.VMEM((LEVELS, GROUP, 8, LANES), jnp.float32),
            pltpu.VMEM((GROUP, 8, LANES), jnp.float32),
            pltpu.VMEM((3, 8, LANES), jnp.float32),
            tile, tile,
            dma((chunks, 3)), dma((chunks, 3)), dma((chunks,)),
            dma((chunks, 5)), dma((chunks, 5)),
            dma((chunks, 3)), dma((chunks, 3)), dma((chunks,)),
            dma((8,)), dma((8,)), dma((4,)), dma((4,)), dma,
        ],
        compiler_params=pltpu.CompilerParams(
            collective_id=0, has_side_effects=True, vmem_limit_bytes=20 << 20),
    )(params, weights)
    return debiased, average, spread


def from_behind(value, axis, steps):
    count = lax.axis_size(axis)
    pairs = [(source, (source + steps) % count) for source in range(count)]
    return lax.ppermute(value, axis, pairs)


def push_round(value, scale, hop):
    received = from_behind((value, scale), "node", hop)
    return (received[0], received[1])


def shards(params, weights):
    node_count = lax.axis_size("node")
    levels = node_count.bit_length() - 1
    scale0 = weights.astype(jnp.float32)
    weighted = scale0[:, None, None] * params.astype(jnp.float32)
    value = weighted
    scale = scale0
    for step in range(ROUNDS):
        hop = 1 << step % levels
        if step == 0:
            raw = from_behind((params, weights.astype(jnp.bfloat16)), "node", hop)
            other_scale = raw[1].astype(jnp.float32)
            other_value = other_scale[:, None, None] * raw[0].astype(jnp.float32)
        else:
            other_value, other_scale = push_round(value, scale, hop)
        value = 0.5 * value + 0.5 * other_value
        scale = 0.5 * scale + 0.5 * other_scale
    debiased = value / scale[:, None, None]
    hidden_units = params.shape[2]
    width = hidden_units // node_count
    local = debiased[0]
    numer, total = lax.psum((weighted[0], jnp.sum(scale0)), "node")
    whole = numer / total
    partial_value = jnp.sum((local - whole) ** 2)[None]
    average = lax.dynamic_slice_in_dim(whole, lax.axis_index("node") * width, width, 1)
    row_count = params.shape[1] * lax.axis_size("blk")
    spread = lax.psum(partial_value, "blk") / (row_count * hidden_units)
    return (debiased, average, spread)


def solution(mesh):
    line = mesh.shape["node"] == GROUP * LEVELS and mesh.shape["blk"] == 2
    return jax.shard_map(
        fused if line else shards,
        mesh=mesh,
        in_specs=(P("node", "blk", None), P("node")),
        out_specs=(P("node", "blk", None), P("blk", "node"), P("node")),
        check_vma=False,
    )
```

```python
import functools

import jax
import jax.numpy as jnp
from jax import lax
from jax.experimental import pallas as pl
from jax.experimental.pallas import tpu as pltpu
from jax.sharding import PartitionSpec as P

ROUNDS = 3
GROUP = 4
LEVELS = 4
SPLIT = 4
LANES = 128
NEIGHBOUR = (1, 0, 3, 2)


def kernel(p_ref, w_ref, out_ref, avg_ref, spread_ref,
           raw_own, raw_a, raw_b, raw_c, q_a, q_b, q_send, dbuf, avgbuf,
           wts, acc, spread_in, spread_part, spread_x,
           near_send, near_recv, own_sem, far_send, far_recv, back_send, back_recv,
           back_own, w_send, w_recv, s_send, s_recv, avg_sem, fore_in, f_send, f_recv):
    node = lax.axis_index("node")
    side = lax.axis_index("blk")
    z = node // GROUP
    r = node % GROUP
    half, core = r // 2, r % 2
    rows, width = raw_own.shape[2], raw_own.shape[3]
    chunks = raw_own.shape[0]
    hidden = p_ref.shape[2]
    row_total = p_ref.shape[1] * lax.axis_size("blk")

    def peer(o):
        y = 1 - half if o & 2 else half
        c = 1 - core if o & 1 else core
        return y * 2 + c

    def dev(zz, rr):
        return {"node": zz * GROUP + rr}

    inner = jnp.logical_and(z >= 1, z <= 2)
    order = [k + half_of for k in range(chunks // 2) for half_of in (0, chunks // 2)]
    mate = 3 - z
    nb = (z // 2) * 2 + 1 - z % 2
    inner_count = (1 - z // 3) * ((z + 2) // 3)

    def remote(src, dst, ssem, rsem, device):
        return pltpu.make_async_remote_copy(
            src_ref=src, dst_ref=dst, send_sem=ssem, recv_sem=rsem,
            device_id=device, device_id_type=pl.DeviceIdType.MESH)

    wts[z, r] = jnp.full((8, LANES), w_ref[0].astype(jnp.float32))
    acc[...] = jnp.zeros_like(acc)

    def own_slice(k):
        return pl.ds((k % SPLIT) * rows, rows)

    def block(k, rr):
        return pl.ds(pl.multiple_of(((k // SPLIT) * GROUP + rr) * width, LANES), width)

    locals_in = []
    for k in range(chunks):
        locals_in.append(pltpu.make_async_copy(
            p_ref.at[0, own_slice(k), block(k, r)], raw_own.at[k, r], own_sem.at[k]))
        locals_in[-1].start()

    barrier = pltpu.get_barrier_semaphore()

    def greet(device):
        pl.semaphore_signal(barrier, inc=1, device_id=device,
                            device_id_type=pl.DeviceIdType.MESH)

    for o in (1, 2, 3):
        greet(dev(z, peer(o)))
    greet({"blk": 1 - side})
    greet(dev(nb, r))

    @pl.when(inner)
    def _():
        greet(dev(mate, r))

    pl.semaphore_wait(barrier, 5 + inner_count)

    def w_near(o):
        return remote(wts.at[z, r], wts.at[z, r], w_send.at[o - 1], w_recv.at[o - 1],
                      dev(z, peer(o)))

    def near(k, o):
        return remote(p_ref.at[0, own_slice(k), block(k, peer(o))], raw_own.at[k, r],
                      near_send.at[k, o - 1], near_recv.at[k, o - 1], dev(z, peer(o)))

    for o in (1, 2, 3):
        w_near(o).start()
    for k in order:
        for o in (2, 3, 1):
            near(k, o).start()

    arrived = set()

    def wait_own(k):
        if k in arrived:
            return
        arrived.add(k)
        locals_in[k].wait()
        for o in (1, 2, 3):
            near(k, o).wait_recv()

    def row(zz, i):
        return wts[zz, i, 0:1, :]

    def f32(ref, k, i, cols):
        return ref[k, i, :, cols].astype(jnp.float32)

    def group_sum(ref, k, zz, cols):
        total = f32(ref, k, 0, cols) * row(zz, 0)
        for i in range(1, GROUP):
            total = total + f32(ref, k, i, cols) * row(zz, i)
        return total

    def columns(j):
        return pl.ds(pl.multiple_of(j * LANES, LANES), LANES)

    def back(k, o):
        return remote(dbuf.at[k, peer(o)], out_ref.at[0, own_slice(k), block(k, r)],
                      back_send.at[k, o - 1], back_recv.at[k, o - 1], dev(z, peer(o)))

    def back_local(k):
        return pltpu.make_async_copy(
            dbuf.at[k, r], out_ref.at[0, own_slice(k), block(k, r)], back_own.at[k])

    def group_weight(zz):
        return row(zz, 0) + row(zz, 1) + row(zz, 2) + row(zz, 3)

    def scales_of(level):
        opp = (level + 2) % LEVELS
        sums = [group_weight((level + 3) % LEVELS)] * GROUP
        for i in range(GROUP):
            for e in range(GROUP):
                if e <= i:
                    sums[i] = sums[i] + row(level, e)
                else:
                    sums[i] = sums[i] + row(opp, e)
        return [1.0 / value for value in sums]

    def is_low(k):
        return k < chunks // 2

    def finish(k, level):
        is_inner = level in (1, 2)
        has_mean = is_low(k) == (level < 2)
        opp, beside, across_level = (level + 2) % 4, NEIGHBOUR[level], 3 - level
        if is_inner:
            raws = {level: raw_own, beside: raw_a, across_level: raw_b, opp: raw_c}
            group_refs = {}
        else:
            raws = {level: raw_own, opp: raw_a}
            group_refs = {beside: q_a, across_level: q_b}
        targets = [level]
        if is_inner and has_mean:
            targets += [across_level, opp]
        scales = {y: scales_of(y) for y in targets}
        whole = 1.0 / (group_weight(0) + group_weight(1) + group_weight(2) + group_weight(3))

        def step(j, sums):
            cols = columns(j)
            seen = {}

            def value(y, i):
                if (y, i) not in seen:
                    seen[y, i] = f32(raws[y], k, i, cols) * row(y, i)
                return seen[y, i]

            def group_of(y):
                if y not in seen:
                    if y in group_refs:
                        seen[y] = group_refs[y][k, :, cols]
                    else:
                        seen[y] = (value(y, 0) + value(y, 1)) + (value(y, 2) + value(y, 3))
                return seen[y]

            if is_inner and sends_opposite(level, k):
                q_send[k, 1, :, cols] = group_of(opp)
            if has_mean:
                mean = (group_of(0) + group_of(1) + group_of(2) + group_of(3)) * whole
                avgbuf[k // SPLIT, own_slice(k), cols] = mean
            fresh = []
            for n, y in enumerate(targets):
                far = (y + 2) % LEVELS
                prior = group_of((y + 3) % LEVELS)
                heads = [value(y, 0)]
                for i in range(1, GROUP):
                    heads.append(heads[-1] + value(y, i))
                tails = [None, None, None, value(far, 3)]
                for i in (2, 1):
                    tails[i] = tails[i + 1] + value(far, i)
                for i in range(GROUP):
                    d = heads[i] + prior
                    if i + 1 < GROUP:
                        d = d + tails[i + 1]
                    d = d * scales[y][i]
                    if n == 0:
                        dbuf[k, i, :, cols] = d
                    if has_mean:
                        gap = d - mean
                        gap = gap * gap
                        part = gap[0:8]
                        for e in range(8, rows, 8):
                            part = part + gap[e:e + 8]
                        fresh.append(sums[len(fresh)] + part)
            return tuple(fresh)

        zero = jnp.zeros((8, LANES), jnp.float32)
        count = GROUP * len(targets) if has_mean else 0
        sums = lax.fori_loop(0, width // LANES, step, (zero,) * count)
        for i in range(count):
            acc[i // GROUP, i % GROUP] += sums[i]

    def share(o):
        return remote(acc.at[0, peer(o)], spread_in.at[o - 1], s_send.at[o - 1],
                      s_recv.at[o - 1], dev(z, peer(o)))

    def send_back(k):
        for o in (2, 3, 1):
            back(k, o).start()
        back_local(k).start()

    def nodes(full):
        return pl.ds(0, GROUP) if full else pl.ds(1, GROUP - 1)

    def sends_opposite(level, k):
        return level == 1 or not is_low(k)

    def sends_own(level, k):
        return level == 2 or is_low(k)

    def to_inner(k, beside):
        return remote(raw_own.at[k], raw_a.at[k], far_send.at[k, 0], far_recv.at[k, 0],
                      dev(beside, r))

    def across(k, source):
        part = nodes(source == 1 or is_low(k))
        return remote(raw_own.at[k, part], raw_b.at[k, part], far_send.at[k, 0],
                      far_recv.at[k, 1], dev(3 - source, r))

    def across_relay(k, source):
        part = nodes(source == 2 or not is_low(k))
        return remote(raw_a.at[k, part], raw_c.at[k, part], far_send.at[k, 1],
                      far_recv.at[k, 2], dev(3 - source, r))

    def outward_relay(k, source):
        part = nodes(is_low(k) == (source == 1))
        return remote(raw_b.at[k, part], raw_a.at[k, part], far_send.at[k, 2],
                      far_recv.at[k, 0], dev(NEIGHBOUR[source], r))

    def outward_q(k, which, source):
        dst = q_b if which else q_a
        return remote(q_send.at[k, which], dst.at[k], far_send.at[k, 3 + which],
                      far_recv.at[k, 3 + which], dev(NEIGHBOUR[source], r))

    def w_copy(level, slot, target):
        return remote(wts.at[level], wts.at[level], w_send.at[slot], w_recv.at[slot],
                      dev(target, r))

    def wait_weights():
        for o in (1, 2, 3):
            w_near(o).wait_recv()

    def foreign(target):
        return remote(acc.at[pl.ds(1, 2)], fore_in, f_send.at[0], f_recv.at[0],
                      dev(target, r))

    def foreign_relay(target):
        return remote(fore_in.at[1], fore_in.at[0], f_send.at[1], f_recv.at[1],
                      dev(target, r))

    def inner_role(level):
        beside, other, opp = NEIGHBOUR[level], 3 - level, (level + 2) % LEVELS
        arrived.clear()

        def group_out(k):
            wait_own(k)
            if not sends_own(level, k):
                return

            def step(j, carry):
                cols = columns(j)
                q_send[k, 0, :, cols] = group_sum(raw_own, k, level, cols)
                return carry

            lax.fori_loop(0, width // LANES, step, 0)
            outward_q(k, 0, level).start()

        wait_weights()
        w_copy(level, 3, beside).start()
        w_copy(level, 4, other).start()
        for t in range(chunks + 2):
            if t < chunks:
                wait_own(order[t])
                across(order[t], level).start()
            for e in ((0,) if t == 0 else (2 * t - 1, 2 * t)):
                if e < chunks:
                    group_out(order[e])
            if t == 1:
                w_copy(beside, 3, beside).wait_recv()
                w_copy(beside, 5, other).start()
                w_copy(level, 4, other).wait_recv()
                w_copy(other, 6, beside).start()
            if 0 <= t - 1 < chunks:
                k = order[t - 1]
                to_inner(k, beside).wait_recv()
                across_relay(k, level).start()
                across(k, other).wait_recv()
                outward_relay(k, level).start()
            if t == 2:
                w_copy(opp, 5, other).wait_recv()
                w_copy(opp, 7, beside).start()
            if 0 <= t - 2 < chunks:
                k = order[t - 2]
                across_relay(k, other).wait_recv()
                finish(k, level)
                if sends_opposite(level, k):
                    outward_q(k, 1, level).start()
                if t == chunks + 1:
                    foreign(other).start()
                send_back(k)
        foreign(other).wait_recv()
        foreign_relay(beside).start()
        acc[0] += fore_in[0]
        for o in (1, 2, 3):
            share(o).start()
        for k in order:
            across(k, level).wait_send()
            across_relay(k, level).wait_send()
            outward_relay(k, level).wait_send()
            if sends_own(level, k):
                outward_q(k, 0, level).wait_send()
            if sends_opposite(level, k):
                outward_q(k, 1, level).wait_send()
        w_copy(level, 3, beside).wait_send()
        w_copy(level, 4, other).wait_send()
        w_copy(beside, 5, other).wait_send()
        w_copy(other, 6, beside).wait_send()
        w_copy(opp, 7, beside).wait_send()
        foreign(other).wait_send()
        foreign_relay(beside).wait_send()

    def outer_role(level):
        beside, other, opp = NEIGHBOUR[level], 3 - level, (level + 2) % LEVELS
        arrived.clear()
        wait_weights()
        w_copy(level, 3, beside).start()
        for k in order:
            wait_own(k)
            to_inner(k, beside).start()
        w_copy(beside, 3, beside).wait_recv()
        w_copy(opp, 6, beside).wait_recv()
        w_copy(other, 7, beside).wait_recv()
        for k in order:
            if sends_own(beside, k):
                outward_q(k, 0, beside).wait_recv()
            outward_relay(k, beside).wait_recv()
            if sends_opposite(beside, k):
                outward_q(k, 1, beside).wait_recv()
            finish(k, level)
            if k == order[-1]:
                foreign_relay(beside).wait_recv()
                acc[0] += fore_in[0]
                for o in (1, 2, 3):
                    share(o).start()
            send_back(k)
        for k in order:
            to_inner(k, beside).wait_send()
        w_copy(level, 3, beside).wait_send()

    for level in range(LEVELS):
        role = inner_role if level in (1, 2) else outer_role
        pl.when(z == level)(functools.partial(role, level))

    average = pltpu.make_async_copy(avgbuf.at[z], avg_ref, avg_sem)
    average.start()

    for o in (1, 2, 3):
        share(o).wait_recv()
    spread_part[...] = acc[0, r] + spread_in[0] + spread_in[1] + spread_in[2]
    swap = remote(spread_part, spread_x, s_send.at[3], s_recv.at[3], {"blk": 1 - side})
    swap.start()
    for k in range(chunks):
        for o in (1, 2, 3):
            near(k, o).wait_send()
            back(k, o).wait()
        back_local(k).wait()
    for o in (1, 2, 3):
        w_near(o).wait_send()
        share(o).wait_send()
    average.wait()
    swap.wait()
    spread_ref[0] = jnp.sum(spread_part[...] + spread_x[...]) / (row_total * hidden)


def fused(params, weights):
    _, rows, hidden = params.shape
    node_count = lax.axis_size("node")
    width = hidden // node_count
    piece = rows // SPLIT
    chunks = LEVELS * SPLIT
    raw = pltpu.VMEM((chunks, GROUP, piece, width), params.dtype)
    q = pltpu.VMEM((chunks, piece, width), jnp.float32)
    tile = pltpu.VMEM((8, LANES), jnp.float32)
    dma = pltpu.SemaphoreType.DMA
    debiased, average, spread = pl.pallas_call(
        kernel,
        out_shape=(
            jax.ShapeDtypeStruct((1, rows, hidden), jnp.float32),
            jax.ShapeDtypeStruct((rows, width), jnp.float32),
            jax.ShapeDtypeStruct((1,), jnp.float32),
        ),
        in_specs=[pl.BlockSpec(memory_space=pltpu.HBM), pl.BlockSpec(memory_space=pltpu.SMEM)],
        out_specs=(pl.BlockSpec(memory_space=pl.ANY), pl.BlockSpec(memory_space=pl.ANY),
                   pl.BlockSpec(memory_space=pltpu.SMEM)),
        scratch_shapes=[
            raw, raw, raw, raw, q, q,
            pltpu.VMEM((chunks, 2, piece, width), jnp.float32),
            pltpu.VMEM((chunks, GROUP, piece, width), jnp.float32),
            pltpu.VMEM((LEVELS, rows, width), jnp.float32),
            pltpu.VMEM((LEVELS, GROUP, 8, LANES), jnp.float32),
            pltpu.VMEM((3, GROUP, 8, LANES), jnp.float32),
            pltpu.VMEM((3, 8, LANES), jnp.float32),
            tile, tile,
            dma((chunks, 3)), dma((chunks, 3)), dma((chunks,)),
            dma((chunks, 5)), dma((chunks, 5)),
            dma((chunks, 3)), dma((chunks, 3)), dma((chunks,)),
            dma((8,)), dma((8,)), dma((4,)), dma((4,)), dma,
            pltpu.VMEM((2, GROUP, 8, LANES), jnp.float32), dma((2,)), dma((2,)),
        ],
        compiler_params=pltpu.CompilerParams(
            collective_id=0, has_side_effects=True, vmem_limit_bytes=20 << 20),
    )(params, weights)
    return debiased, average, spread


def from_behind(value, axis, steps):
    count = lax.axis_size(axis)
    pairs = [(source, (source + steps) % count) for source in range(count)]
    return lax.ppermute(value, axis, pairs)


def push_round(value, scale, hop):
    received = from_behind((value, scale), "node", hop)
    return (received[0], received[1])


def shards(params, weights):
    node_count = lax.axis_size("node")
    levels = node_count.bit_length() - 1
    scale0 = weights.astype(jnp.float32)
    weighted = scale0[:, None, None] * params.astype(jnp.float32)
    value = weighted
    scale = scale0
    for step in range(ROUNDS):
        hop = 1 << step % levels
        if step == 0:
            raw = from_behind((params, weights.astype(jnp.bfloat16)), "node", hop)
            other_scale = raw[1].astype(jnp.float32)
            other_value = other_scale[:, None, None] * raw[0].astype(jnp.float32)
        else:
            other_value, other_scale = push_round(value, scale, hop)
        value = 0.5 * value + 0.5 * other_value
        scale = 0.5 * scale + 0.5 * other_scale
    debiased = value / scale[:, None, None]
    hidden_units = params.shape[2]
    width = hidden_units // node_count
    local = debiased[0]
    numer, total = lax.psum((weighted[0], jnp.sum(scale0)), "node")
    whole = numer / total
    partial_value = jnp.sum((local - whole) ** 2)[None]
    average = lax.dynamic_slice_in_dim(whole, lax.axis_index("node") * width, width, 1)
    row_count = params.shape[1] * lax.axis_size("blk")
    spread = lax.psum(partial_value, "blk") / (row_count * hidden_units)
    return (debiased, average, spread)


def solution(mesh):
    line = mesh.shape["node"] == GROUP * LEVELS and mesh.shape["blk"] == 2
    return jax.shard_map(
        fused if line else shards,
        mesh=mesh,
        in_specs=(P("node", "blk", None), P("node")),
        out_specs=(P("node", "blk", None), P("blk", "node"), P("node")),
        check_vma=False,
    )
```

```python
import functools

import jax
import jax.numpy as jnp
from jax import lax
from jax.experimental import pallas as pl
from jax.experimental.pallas import tpu as pltpu
from jax.sharding import PartitionSpec as P

ROUNDS = 3
GROUP = 4
LEVELS = 4
SPLIT = 4
LANES = 128
NEIGHBOUR = (1, 0, 3, 2)


def kernel(p_ref, w_ref, out_ref, avg_ref, spread_ref,
           raw_own, raw_a, raw_b, raw_c, q_a, q_b, q_send, dbuf, avgbuf,
           wts, acc, spread_in, spread_part, spread_x,
           near_send, near_recv, own_sem, far_send, far_recv, back_send, back_recv,
           back_own, w_send, w_recv, s_send, s_recv, avg_sem, fore_in, f_send, f_recv):
    node = lax.axis_index("node")
    side = lax.axis_index("blk")
    z = node // GROUP
    r = node % GROUP
    half, core = r // 2, r % 2
    rows, width = raw_own.shape[2], raw_own.shape[3]
    chunks = raw_own.shape[0]
    hidden = p_ref.shape[2]
    row_total = p_ref.shape[1] * lax.axis_size("blk")

    def peer(o):
        y = 1 - half if o & 2 else half
        c = 1 - core if o & 1 else core
        return y * 2 + c

    def dev(zz, rr):
        return {"node": zz * GROUP + rr}

    inner = jnp.logical_and(z >= 1, z <= 2)
    order = [k + half_of for k in range(chunks // 2) for half_of in (0, chunks // 2)]
    mate = 3 - z
    nb = (z // 2) * 2 + 1 - z % 2
    inner_count = (1 - z // 3) * ((z + 2) // 3)

    def remote(src, dst, ssem, rsem, device):
        return pltpu.make_async_remote_copy(
            src_ref=src, dst_ref=dst, send_sem=ssem, recv_sem=rsem,
            device_id=device, device_id_type=pl.DeviceIdType.MESH)

    wts[z, r] = jnp.full((8, LANES), w_ref[0].astype(jnp.float32))
    acc[...] = jnp.zeros_like(acc)

    def own_slice(k):
        return pl.ds((k % SPLIT) * rows, rows)

    def block(k, rr):
        return pl.ds(pl.multiple_of(((k // SPLIT) * GROUP + rr) * width, LANES), width)

    locals_in = []
    for k in range(chunks):
        locals_in.append(pltpu.make_async_copy(
            p_ref.at[0, own_slice(k), block(k, r)], raw_own.at[k, r], own_sem.at[k]))
        locals_in[-1].start()

    barrier = pltpu.get_barrier_semaphore()

    def greet(device):
        pl.semaphore_signal(barrier, inc=1, device_id=device,
                            device_id_type=pl.DeviceIdType.MESH)

    for o in (1, 2, 3):
        greet(dev(z, peer(o)))
    greet({"blk": 1 - side})
    greet(dev(nb, r))

    @pl.when(inner)
    def _():
        greet(dev(mate, r))

    pl.semaphore_wait(barrier, 5 + inner_count)

    def w_near(o):
        return remote(wts.at[z, r], wts.at[z, r], w_send.at[o - 1], w_recv.at[o - 1],
                      dev(z, peer(o)))

    def near(k, o):
        return remote(p_ref.at[0, own_slice(k), block(k, peer(o))], raw_own.at[k, r],
                      near_send.at[k, o - 1], near_recv.at[k, o - 1], dev(z, peer(o)))

    for o in (1, 2, 3):
        w_near(o).start()
    for k in order:
        for o in (2, 3, 1):
            near(k, o).start()

    arrived = set()

    def wait_own(k):
        if k in arrived:
            return
        arrived.add(k)
        locals_in[k].wait()
        for o in (1, 2, 3):
            near(k, o).wait_recv()

    def row(zz, i):
        return wts[zz, i, 0:1, :]

    def f32(ref, k, i, cols):
        return ref[k, i, :, cols].astype(jnp.float32)

    def group_sum(ref, k, zz, cols):
        total = f32(ref, k, 0, cols) * row(zz, 0)
        for i in range(1, GROUP):
            total = total + f32(ref, k, i, cols) * row(zz, i)
        return total

    def columns(j):
        return pl.ds(pl.multiple_of(j * LANES, LANES), LANES)

    def back(k, o):
        return remote(dbuf.at[k, peer(o)], out_ref.at[0, own_slice(k), block(k, r)],
                      back_send.at[k, o - 1], back_recv.at[k, o - 1], dev(z, peer(o)))

    def back_local(k):
        return pltpu.make_async_copy(
            dbuf.at[k, r], out_ref.at[0, own_slice(k), block(k, r)], back_own.at[k])

    def group_weight(zz):
        return row(zz, 0) + row(zz, 1) + row(zz, 2) + row(zz, 3)

    def scales_of(level):
        opp = (level + 2) % LEVELS
        sums = [group_weight((level + 3) % LEVELS)] * GROUP
        for i in range(GROUP):
            for e in range(GROUP):
                if e <= i:
                    sums[i] = sums[i] + row(level, e)
                else:
                    sums[i] = sums[i] + row(opp, e)
        return [1.0 / value for value in sums]

    def is_low(k):
        return k < chunks // 2

    def finish(k, level):
        is_inner = level in (1, 2)
        has_mean = is_low(k) == (level < 2)
        opp, beside, across_level = (level + 2) % 4, NEIGHBOUR[level], 3 - level
        if is_inner:
            raws = {level: raw_own, beside: raw_a, across_level: raw_b, opp: raw_c}
            group_refs = {}
        else:
            raws = {level: raw_own, opp: raw_a}
            group_refs = {beside: q_a, across_level: q_b}
        targets = [level]
        if is_inner and has_mean:
            targets += [across_level, opp]
        scales = {y: scales_of(y) for y in targets}
        whole = 1.0 / (group_weight(0) + group_weight(1) + group_weight(2) + group_weight(3))

        def step(j, sums):
            cols = columns(j)
            seen = {}

            def value(y, i):
                if (y, i) not in seen:
                    seen[y, i] = f32(raws[y], k, i, cols) * row(y, i)
                return seen[y, i]

            def group_of(y):
                if y not in seen:
                    if y in group_refs:
                        seen[y] = group_refs[y][k, :, cols]
                    else:
                        seen[y] = (value(y, 0) + value(y, 1)) + (value(y, 2) + value(y, 3))
                return seen[y]

            if is_inner and sends_opposite(level, k):
                q_send[k, 1, :, cols] = group_of(opp)
            if has_mean:
                mean = (group_of(0) + group_of(1) + group_of(2) + group_of(3)) * whole
                avgbuf[k // SPLIT, own_slice(k), cols] = mean
            fresh = []
            for n, y in enumerate(targets):
                far = (y + 2) % LEVELS
                prior = group_of((y + 3) % LEVELS)
                heads = [value(y, 0)]
                for i in range(1, GROUP):
                    heads.append(heads[-1] + value(y, i))
                tails = [None, None, None, value(far, 3)]
                for i in (2, 1):
                    tails[i] = tails[i + 1] + value(far, i)
                for i in range(GROUP):
                    d = heads[i] + prior
                    if i + 1 < GROUP:
                        d = d + tails[i + 1]
                    d = d * scales[y][i]
                    if n == 0:
                        dbuf[k, i, :, cols] = d
                    if has_mean:
                        gap = d - mean
                        gap = gap * gap
                        part = gap[0:8]
                        for e in range(8, rows, 8):
                            part = part + gap[e:e + 8]
                        fresh.append(sums[len(fresh)] + part)
            return tuple(fresh)

        zero = jnp.zeros((8, LANES), jnp.float32)
        count = GROUP * len(targets) if has_mean else 0
        sums = lax.fori_loop(0, width // LANES, step, (zero,) * count)
        for i in range(count):
            acc[i // GROUP, i % GROUP] += sums[i]

    def share(o):
        return remote(acc.at[0, peer(o)], spread_in.at[o - 1], s_send.at[o - 1],
                      s_recv.at[o - 1], dev(z, peer(o)))

    def send_back(k):
        for o in (2, 3, 1):
            back(k, o).start()
        back_local(k).start()

    def nodes(full):
        return pl.ds(0, GROUP) if full else pl.ds(1, GROUP - 1)

    def sends_opposite(level, k):
        return level == 1 or not is_low(k)

    def sends_own(level, k):
        return level == 2 or is_low(k)

    def to_inner(k, beside):
        return remote(raw_own.at[k], raw_a.at[k], far_send.at[k, 0], far_recv.at[k, 0],
                      dev(beside, r))

    def across(k, source):
        part = nodes(source == 1 or is_low(k))
        return remote(raw_own.at[k, part], raw_b.at[k, part], far_send.at[k, 0],
                      far_recv.at[k, 1], dev(3 - source, r))

    def across_relay(k, source):
        part = nodes(source == 2 or not is_low(k))
        return remote(raw_a.at[k, part], raw_c.at[k, part], far_send.at[k, 1],
                      far_recv.at[k, 2], dev(3 - source, r))

    def outward_relay(k, source):
        part = nodes(is_low(k) == (source == 1))
        return remote(raw_b.at[k, part], raw_a.at[k, part], far_send.at[k, 2],
                      far_recv.at[k, 0], dev(NEIGHBOUR[source], r))

    def outward_q(k, which, source):
        dst = q_b if which else q_a
        return remote(q_send.at[k, which], dst.at[k], far_send.at[k, 3 + which],
                      far_recv.at[k, 3 + which], dev(NEIGHBOUR[source], r))

    def w_copy(level, slot, target):
        return remote(wts.at[level], wts.at[level], w_send.at[slot], w_recv.at[slot],
                      dev(target, r))

    def wait_weights():
        for o in (1, 2, 3):
            w_near(o).wait_recv()

    def foreign(target):
        return remote(acc.at[pl.ds(1, 2)], fore_in, f_send.at[0], f_recv.at[0],
                      dev(target, r))

    def foreign_relay(target):
        return remote(fore_in.at[1], fore_in.at[0], f_send.at[1], f_recv.at[1],
                      dev(target, r))

    def inner_role(level):
        beside, other, opp = NEIGHBOUR[level], 3 - level, (level + 2) % LEVELS
        arrived.clear()

        def group_out(k):
            wait_own(k)
            if not sends_own(level, k):
                return

            def step(j, carry):
                cols = columns(j)
                q_send[k, 0, :, cols] = group_sum(raw_own, k, level, cols)
                return carry

            lax.fori_loop(0, width // LANES, step, 0)
            outward_q(k, 0, level).start()

        wait_weights()
        w_copy(level, 3, beside).start()
        w_copy(level, 4, other).start()
        for t in range(chunks + 2):
            for e in ((0, 1) if t == 0 else (t + 1,)):
                if e < chunks:
                    wait_own(order[e])
                    across(order[e], level).start()
            for e in ((0,) if t == 0 else (2 * t - 1, 2 * t)):
                if e < chunks:
                    group_out(order[e])
            if t == 1:
                w_copy(beside, 3, beside).wait_recv()
                w_copy(beside, 5, other).start()
                w_copy(level, 4, other).wait_recv()
                w_copy(other, 6, beside).start()
            if 0 <= t - 1 < chunks:
                k = order[t - 1]
                to_inner(k, beside).wait_recv()
                across_relay(k, level).start()
                across(k, other).wait_recv()
                outward_relay(k, level).start()
            if t == 2:
                w_copy(opp, 5, other).wait_recv()
                w_copy(opp, 7, beside).start()
            if 0 <= t - 2 < chunks:
                k = order[t - 2]
                across_relay(k, other).wait_recv()
                finish(k, level)
                if sends_opposite(level, k):
                    outward_q(k, 1, level).start()
                if t == chunks + 1:
                    foreign(other).start()
                send_back(k)
        foreign(other).wait_recv()
        foreign_relay(beside).start()
        acc[0] += fore_in[0]
        for o in (1, 2, 3):
            share(o).start()
        for k in order:
            across(k, level).wait_send()
            across_relay(k, level).wait_send()
            outward_relay(k, level).wait_send()
            if sends_own(level, k):
                outward_q(k, 0, level).wait_send()
            if sends_opposite(level, k):
                outward_q(k, 1, level).wait_send()
        w_copy(level, 3, beside).wait_send()
        w_copy(level, 4, other).wait_send()
        w_copy(beside, 5, other).wait_send()
        w_copy(other, 6, beside).wait_send()
        w_copy(opp, 7, beside).wait_send()
        foreign(other).wait_send()
        foreign_relay(beside).wait_send()

    def outer_role(level):
        beside, other, opp = NEIGHBOUR[level], 3 - level, (level + 2) % LEVELS
        arrived.clear()
        wait_weights()
        w_copy(level, 3, beside).start()
        for k in order:
            wait_own(k)
            to_inner(k, beside).start()
        w_copy(beside, 3, beside).wait_recv()
        w_copy(opp, 6, beside).wait_recv()
        w_copy(other, 7, beside).wait_recv()
        for k in order:
            if sends_own(beside, k):
                outward_q(k, 0, beside).wait_recv()
            outward_relay(k, beside).wait_recv()
            if sends_opposite(beside, k):
                outward_q(k, 1, beside).wait_recv()
            finish(k, level)
            if k == order[-1]:
                foreign_relay(beside).wait_recv()
                acc[0] += fore_in[0]
                for o in (1, 2, 3):
                    share(o).start()
            send_back(k)
        for k in order:
            to_inner(k, beside).wait_send()
        w_copy(level, 3, beside).wait_send()

    for level in range(LEVELS):
        role = inner_role if level in (1, 2) else outer_role
        pl.when(z == level)(functools.partial(role, level))

    average = pltpu.make_async_copy(avgbuf.at[z], avg_ref, avg_sem)
    average.start()

    for o in (1, 2, 3):
        share(o).wait_recv()
    spread_part[...] = acc[0, r] + spread_in[0] + spread_in[1] + spread_in[2]
    swap = remote(spread_part, spread_x, s_send.at[3], s_recv.at[3], {"blk": 1 - side})
    swap.start()
    for k in range(chunks):
        for o in (1, 2, 3):
            near(k, o).wait_send()
            back(k, o).wait()
        back_local(k).wait()
    for o in (1, 2, 3):
        w_near(o).wait_send()
        share(o).wait_send()
    average.wait()
    swap.wait()
    spread_ref[0] = jnp.sum(spread_part[...] + spread_x[...]) / (row_total * hidden)


def fused(params, weights):
    _, rows, hidden = params.shape
    node_count = lax.axis_size("node")
    width = hidden // node_count
    piece = rows // SPLIT
    chunks = LEVELS * SPLIT
    raw = pltpu.VMEM((chunks, GROUP, piece, width), params.dtype)
    q = pltpu.VMEM((chunks, piece, width), jnp.float32)
    tile = pltpu.VMEM((8, LANES), jnp.float32)
    dma = pltpu.SemaphoreType.DMA
    debiased, average, spread = pl.pallas_call(
        kernel,
        out_shape=(
            jax.ShapeDtypeStruct((1, rows, hidden), jnp.float32),
            jax.ShapeDtypeStruct((rows, width), jnp.float32),
            jax.ShapeDtypeStruct((1,), jnp.float32),
        ),
        in_specs=[pl.BlockSpec(memory_space=pltpu.HBM), pl.BlockSpec(memory_space=pltpu.SMEM)],
        out_specs=(pl.BlockSpec(memory_space=pl.ANY), pl.BlockSpec(memory_space=pl.ANY),
                   pl.BlockSpec(memory_space=pltpu.SMEM)),
        scratch_shapes=[
            raw, raw, raw, raw, q, q,
            pltpu.VMEM((chunks, 2, piece, width), jnp.float32),
            pltpu.VMEM((chunks, GROUP, piece, width), jnp.float32),
            pltpu.VMEM((LEVELS, rows, width), jnp.float32),
            pltpu.VMEM((LEVELS, GROUP, 8, LANES), jnp.float32),
            pltpu.VMEM((3, GROUP, 8, LANES), jnp.float32),
            pltpu.VMEM((3, 8, LANES), jnp.float32),
            tile, tile,
            dma((chunks, 3)), dma((chunks, 3)), dma((chunks,)),
            dma((chunks, 5)), dma((chunks, 5)),
            dma((chunks, 3)), dma((chunks, 3)), dma((chunks,)),
            dma((8,)), dma((8,)), dma((4,)), dma((4,)), dma,
            pltpu.VMEM((2, GROUP, 8, LANES), jnp.float32), dma((2,)), dma((2,)),
        ],
        compiler_params=pltpu.CompilerParams(
            collective_id=0, has_side_effects=True, vmem_limit_bytes=20 << 20),
    )(params, weights)
    return debiased, average, spread


def from_behind(value, axis, steps):
    count = lax.axis_size(axis)
    pairs = [(source, (source + steps) % count) for source in range(count)]
    return lax.ppermute(value, axis, pairs)


def push_round(value, scale, hop):
    received = from_behind((value, scale), "node", hop)
    return (received[0], received[1])


def shards(params, weights):
    node_count = lax.axis_size("node")
    levels = node_count.bit_length() - 1
    scale0 = weights.astype(jnp.float32)
    weighted = scale0[:, None, None] * params.astype(jnp.float32)
    value = weighted
    scale = scale0
    for step in range(ROUNDS):
        hop = 1 << step % levels
        if step == 0:
            raw = from_behind((params, weights.astype(jnp.bfloat16)), "node", hop)
            other_scale = raw[1].astype(jnp.float32)
            other_value = other_scale[:, None, None] * raw[0].astype(jnp.float32)
        else:
            other_value, other_scale = push_round(value, scale, hop)
        value = 0.5 * value + 0.5 * other_value
        scale = 0.5 * scale + 0.5 * other_scale
    debiased = value / scale[:, None, None]
    hidden_units = params.shape[2]
    width = hidden_units // node_count
    local = debiased[0]
    numer, total = lax.psum((weighted[0], jnp.sum(scale0)), "node")
    whole = numer / total
    partial_value = jnp.sum((local - whole) ** 2)[None]
    average = lax.dynamic_slice_in_dim(whole, lax.axis_index("node") * width, width, 1)
    row_count = params.shape[1] * lax.axis_size("blk")
    spread = lax.psum(partial_value, "blk") / (row_count * hidden_units)
    return (debiased, average, spread)


def solution(mesh):
    line = mesh.shape["node"] == GROUP * LEVELS and mesh.shape["blk"] == 2
    return jax.shard_map(
        fused if line else shards,
        mesh=mesh,
        in_specs=(P("node", "blk", None), P("node")),
        out_specs=(P("node", "blk", None), P("blk", "node"), P("node")),
        check_vma=False,
    )
```
